256 devices in a mesh: term: 16 (over z, y_hi), sec: 16 (over y_lo, x, core).
Axes of the slice: x: 4, y: 4 (y_hi: 2, y_lo: 2; y = y_hi * 2 + y_lo), z: 8, core: 2. Of those that a mesh axis runs over, the one named last changes fastest.
Arguments:
- state: bfloat16 [16, 768, 768], P('sec'), may hold values from -6 to 6
- left_environment: bfloat16 [16, 16, 768, 768], P('term', 'sec'), may hold values from -0.21875 to 0.21875
- right_environment: bfloat16 [16, 16, 768, 768], P('term', 'sec'), may hold values from -0.21875 to 0.21875
- site_blocks: bfloat16 [16, 768, 768], P('sec'), may hold values from -3 to 3
- sector_sizes: int32 [16], replicated, may hold values from 192 to 768, as said below
- term_shift: int32 [16], P('term'), may hold values from -1 to 1
Outputs:
- applied: float32 [16, 768, 768], P('sec', 'term')
- new_left: bfloat16 [16, 16, 768, 768], P('term', 'sec')
The draws below stay inside these ranges and needn't reach their ends.
Inputs may be any that keep to these rules, and one draw needn't show every extreme that they name: `sector_sizes`: every sector holds at least 192 states and the largest sector holds exactly 768.
All inputs are finite; a program needn't handle non-finite values.
Results may differ from the reference program's by a relative error of at most 0.0049.
Values may be sent and summed in bfloat16 or wider, within the bound.
No kernel may reach another device: no remote copies, remote signals or barrier semaphores. Data moves between devices by JAX's collectives and lax.ppermute only.
A program may use at most 64 MiB of HBM per device.

```python
import jax
import jax.numpy as jnp
from jax import lax

M = 768
NSEC = 16
NTERM = 16


def draw_sector_sizes(key, part):
    first_key, second_key = jax.random.split(jax.random.fold_in(key, 11))
    counts = jax.random.randint(first_key, (NSEC,), M // 4, M + 1)
    largest = jax.random.randint(second_key, (), 0, NSEC)
    return counts.at[largest].set(M).astype(jnp.int32)


def touch_ends(entries, stream_key, least, top_value):
    longest = entries.shape.index(max(entries.shape))
    spots = []
    for shift in (0, 1):
        where = [jax.random.randint(jax.random.fold_in(stream_key, axis), (), 0, length) for axis, length in enumerate(entries.shape)]
        where[longest] = (where[longest] + shift) % entries.shape[longest]
        spots.append(tuple(where))
    return entries.at[spots[0]].set(least).at[spots[1]].set(top_value)


def block_levels(stream_key, dims, cuts, least, high):
    loudness, own = 1.0, jax.random.fold_in(stream_key, 6)
    for dim, blocks in cuts:
        steps = jnp.exp(jax.random.uniform(jax.random.fold_in(own, dim), (blocks,), jnp.float32, least / len(cuts), high / len(cuts)))
        loudness = loudness * jnp.repeat(steps, dims[dim] // blocks).reshape([-1 if axis == dim else 1 for axis in range(len(dims))])
    return loudness


def noise(key, shape, width, most, cuts=(), held_as=jnp.bfloat16):
    level = block_levels(key, shape, cuts, -0.22, 0.18) if cuts else 1.0
    values = jax.random.normal(key, shape, jnp.float32) * width * level
    return jnp.minimum(jnp.maximum(values, -most), most).astype(held_as)


def setup_inputs(seed: int = 0) -> dict:
    streams_of = jax.random.split(jax.random.key(seed), 7)
    return {
        "state": noise(streams_of[0], (NSEC, M, M), 1.0, 6.0, ((0, 16),)),
        "left_environment": noise(streams_of[1], (NTERM, NSEC, M, M), M ** -0.5, 0.21875, ((0, 16), (1, 16))),
        "right_environment": noise(streams_of[2], (NTERM, NSEC, M, M), M ** -0.5, 0.21875, ((0, 16), (1, 16))),
        "site_blocks": noise(streams_of[3], (NSEC, M, M), (M ** -0.25), 3.0, ((0, 16),)),
        "sector_sizes": draw_sector_sizes(jax.random.fold_in(streams_of[6], 71), 0),
        "term_shift": touch_ends(jax.random.randint(streams_of[5], (NTERM,), -1, 2), jax.random.fold_in(streams_of[5], 1), -1, 1).astype(jnp.int32),
    }


def shifted(padded, charge_shift):
    return lax.dynamic_slice_in_dim(padded, (charge_shift + 1).astype(jnp.int32), NSEC, 0)


def reference(state, left_environment, right_environment, site_blocks, sector_sizes, term_shift):
    row_index = jnp.arange(M, dtype=jnp.int32)
    valid_rows = (row_index[None, :] < sector_sizes[:, None]).astype(jnp.float32)
    both = valid_rows[:, :, None] * valid_rows[:, None, :]
    masked_state = state.astype(jnp.float32) * both
    masked_site = site_blocks.astype(jnp.float32) * both
    empty = jnp.zeros((1, M, M), jnp.float32)
    state_padded = jnp.concatenate([empty, masked_state, empty], axis=0)
    site_padded = jnp.concatenate([empty, masked_site, empty], axis=0)
    valid_padded = jnp.concatenate([jnp.zeros((1, M), jnp.float32), valid_rows, jnp.zeros((1, M), jnp.float32)], axis=0)
    highest = lax.Precision.HIGHEST

    def one_term(total, inputs):
        left_term, right_term, charge_shift = inputs
        source_valid = shifted(valid_padded, charge_shift)
        source_state = shifted(state_padded, charge_shift)
        source_site = shifted(site_padded, charge_shift)
        left_masked = left_term.astype(jnp.float32) * valid_rows[:, :, None] * source_valid[:, None, :]
        right_masked = right_term.astype(jnp.float32) * source_valid[:, :, None] * valid_rows[:, None, :]
        mixed_block = jnp.einsum("sij,sjk->sik", source_state, right_masked, precision=highest)
        mixed_block = mixed_block.astype(jnp.bfloat16).astype(jnp.float32)
        partial_rows = jnp.einsum("sij,sjk->sik", left_masked, mixed_block, precision=highest)
        carried = jnp.einsum("sij,sjk->sik", left_masked, source_site, precision=highest)
        carried = carried.astype(jnp.bfloat16).astype(jnp.float32)
        renewed = jnp.einsum("sji,sjk->sik", masked_site, carried, precision=highest).astype(jnp.bfloat16)
        return total + partial_rows, renewed

    applied, new_left = lax.scan(one_term, jnp.zeros((NSEC, M, M), jnp.float32), (left_environment, right_environment, term_shift))
    return applied, new_left
```

```python
import functools

import jax
import jax.numpy as jnp
from jax import lax
from jax.experimental import pallas as pl
from jax.experimental.pallas import tpu as pltpu
from jax.sharding import PartitionSpec as P


WIDTH = 768
TERMS = 16
SECTORS = 16
PIECE = WIDTH // TERMS
CHUNKS = 2
SPAN = WIDTH // CHUNKS
RINGS = TERMS // 2
JUMPS = (1, -1, 3)
BF16 = jnp.bfloat16
F32 = jnp.float32
VMEM = pl.BlockSpec(memory_space=pltpu.VMEM)
SMEM = pl.BlockSpec(memory_space=pltpu.SMEM)


def partner(stage, term, sector):
    ring, half = term // 2, term % 2
    if stage == 3:
        return 2 * ring + 1 - half
    sign = 1 - 2 * ((ring + sector) % 2)
    return 2 * ((ring + sign * JUMPS[stage] + RINGS) % RINGS) + half


def swap(block, where):
    route = []
    for term in range(TERMS):
        for sector in range(SECTORS):
            other = where(term, sector)
            if other is not None:
                route.append((term * SECTORS + sector, other[0] * SECTORS + other[1]))
    return lax.ppermute(block, ("term", "sec"), route)


def pair_sector(term, sector):
    return term, sector ^ 1


def next_sector(term, sector):
    other = sector + 1 if sector % 2 else sector - 1
    return (term, other) if 0 <= other < SECTORS else None


def stage_route(stage):
    return lambda term, sector: (partner(stage, term, sector), sector)


def sizes_here(sizes_ref, shift_ref):
    sector = lax.axis_index("sec")
    source = sector + shift_ref[0]
    inside = (source >= 0) & (source < SECTORS)
    source_size = jnp.where(inside, sizes_ref[jnp.clip(source, 0, SECTORS - 1)], 0)
    return sizes_ref[sector], source_size


def ones_below(size, start, count, dim):
    shape = (count, 1) if dim == 0 else (1, count)
    index = lax.broadcasted_iota(jnp.int32, shape, dim) + start
    return jnp.where(index < size, 1.0, 0.0).astype(BF16)


def piece_at(slot):
    term, sector = lax.axis_index("term"), lax.axis_index("sec")
    for stage in range(4):
        if not (slot >> (3 - stage)) & 1:
            term = partner(stage, term, sector)
    return term


def prepare_kernel(sizes_ref, shift_ref, left_ref, right_ref, site_ref, left_out, right_out, site_out):
    own, source = sizes_here(sizes_ref, shift_ref)
    own_columns = ones_below(own, 0, WIDTH, 1)
    source_columns = ones_below(source, 0, WIDTH, 1)
    for slot in range(TERMS):
        start = pl.multiple_of(piece_at(slot) * PIECE, 16)
        here = pl.ds(slot * PIECE, PIECE)
        rows = ones_below(own, start, PIECE, 0)
        left_out[here, :] = left_ref[pl.ds(start, PIECE), :] * rows * source_columns
        site_out[here, :] = site_ref[pl.ds(start, PIECE), :] * own_columns
        source_rows = ones_below(source, slot * PIECE, PIECE, 0)
        right_out[here, :] = right_ref[here, :] * source_rows * own_columns


def chosen(shift_ref, own_ref, pair_ref, next_ref):
    shift = shift_ref[0]
    even = lax.axis_index("sec") % 2 == 0
    from_pair = jnp.where(even, shift == 1, shift == -1)
    return jnp.where(shift == 0, own_ref[...], jnp.where(from_pair, pair_ref[...], next_ref[...]))


def apply_kernel(chunk, shift_ref, own_ref, pair_ref, next_ref, right_ref, left_ref, send_ref, keep_ref):
    source = chosen(shift_ref, own_ref, pair_ref, next_ref)
    columns = pl.ds(chunk * SPAN, SPAN)
    mixed = jnp.dot(source, right_ref[:, columns], preferred_element_type=F32).astype(BF16)
    half = WIDTH // 2
    send_ref[...] = jnp.dot(left_ref[:half, :], mixed, preferred_element_type=F32).astype(BF16)
    keep_ref[...] = jnp.dot(left_ref[half:, :], mixed, preferred_element_type=F32)


def merge_kernel(keep_ref, got_ref, send_out, keep_out):
    half = keep_ref.shape[0] // 2
    send_out[...] = (keep_ref[:half, :] + got_ref[:half, :].astype(F32)).astype(BF16)
    keep_out[...] = keep_ref[half:, :] + got_ref[half:, :].astype(F32)


def finish_kernel(*refs):
    out = refs[-1]
    for chunk in range(CHUNKS):
        keep, got = refs[2 * chunk : 2 * chunk + 2]
        out[:, chunk * SPAN : (chunk + 1) * SPAN] = keep[...] + got[...].astype(F32)


def renew_kernel(sizes_ref, shift_ref, own_ref, pair_ref, next_ref, left_ref, site_ref, out_ref):
    _, source_size = sizes_here(sizes_ref, shift_ref)
    source = chosen(shift_ref, own_ref, pair_ref, next_ref)
    carried = jnp.dot(left_ref[...], source, preferred_element_type=F32).astype(BF16)
    carried = carried * ones_below(source_size, 0, WIDTH, 1)
    renewed = lax.dot_general(
        site_ref[...], carried, (((0,), (0,)), ((), ())), preferred_element_type=F32
    )
    out_ref[...] = renewed.astype(BF16)


def room(mebibytes):
    return pltpu.CompilerParams(vmem_limit_bytes=mebibytes * 1024 * 1024)


def cost(flops, moved):
    return pl.CostEstimate(flops=flops, bytes_accessed=moved, transcendentals=0)


def shards(state, left_environment, right_environment, site_blocks, sector_sizes, term_shift):
    square = jax.ShapeDtypeStruct((WIDTH, WIDTH), BF16)
    state_own, site_own = state[0], site_blocks[0]
    state_next = swap(state_own, next_sector)
    state_pair = swap(state_own, pair_sector)
    site_next = swap(site_own, next_sector)
    site_pair = swap(site_own, pair_sector)
    left, right, site = pl.pallas_call(
        prepare_kernel,
        out_shape=(square, square, square),
        in_specs=[SMEM, SMEM, VMEM, VMEM, VMEM],
        out_specs=(VMEM, VMEM, VMEM),
        cost_estimate=cost(6_000_000, 7_000_000),
        compiler_params=room(20),
        name="prepare",
    )(sector_sizes, term_shift, left_environment[0, 0], right_environment[0, 0], site_own)
    flow = []
    for chunk in range(CHUNKS):
        half = WIDTH // 2
        flow.append(
            pl.pallas_call(
                functools.partial(apply_kernel, chunk),
                out_shape=(
                    jax.ShapeDtypeStruct((half, SPAN), BF16),
                    jax.ShapeDtypeStruct((half, SPAN), F32),
                ),
                in_specs=[SMEM] + [VMEM] * 5,
                out_specs=(VMEM, VMEM),
                cost_estimate=cost(4 * WIDTH * WIDTH * SPAN, 6_000_000),
                compiler_params=room(20),
        name="apply",
            )(term_shift, state_own, state_pair, state_next, right, left)
        )
    for stage in range(4):
        arrived = [(keep, swap(send, stage_route(stage))) for send, keep in flow]
        if stage == 3:
            break
        flow = []
        for keep, got in arrived:
            rows = keep.shape[0] // 2
            flow.append(
                pl.pallas_call(
                    merge_kernel,
                    out_shape=(
                        jax.ShapeDtypeStruct((rows, SPAN), BF16),
                        jax.ShapeDtypeStruct((rows, SPAN), F32),
                    ),
                    in_specs=[VMEM, VMEM],
                    out_specs=(VMEM, VMEM),
                    cost_estimate=cost(2 * rows * SPAN, 8 * rows * SPAN),
                    compiler_params=room(6),
        name="merge",
                )(keep, got)
            )
    applied = pl.pallas_call(
        finish_kernel,
        out_shape=jax.ShapeDtypeStruct((PIECE, WIDTH), F32),
        in_specs=[VMEM] * (2 * CHUNKS),
        out_specs=VMEM,
        cost_estimate=cost(PIECE * WIDTH, 8 * PIECE * WIDTH),
        compiler_params=room(4),
        name="finish",
    )(*[array for pair in arrived for array in pair])
    renewed = pl.pallas_call(
        renew_kernel,
        out_shape=square,
        in_specs=[SMEM, SMEM] + [VMEM] * 5,
        out_specs=VMEM,
        cost_estimate=cost(4 * WIDTH * WIDTH * WIDTH, 7_000_000),
        compiler_params=room(20),
        name="renew",
    )(sector_sizes, term_shift, site_own, site_pair, site_next, left, site)
    return applied[None], renewed[None, None]


def solution(mesh):
    placed = (
        P("sec", None, None),
        P("term", "sec", None, None),
        P("term", "sec", None, None),
        P("sec", None, None),
        P(),
        P("term"),
    )
    return jax.shard_map(
        shards,
        mesh=mesh,
        in_specs=placed,
        out_specs=(P("sec", "term", None), P("term", "sec", None, None)),
        check_vma=False,
    )
```

```python
import functools

import jax
import jax.numpy as jnp
from jax import lax
from jax.experimental import pallas as pl
from jax.experimental.pallas import tpu as pltpu
from jax.sharding import PartitionSpec as P


WIDTH = 768
TERMS = 16
SECTORS = 16
PIECE = WIDTH // TERMS
CHUNKS = 2
SPAN = WIDTH // CHUNKS
RINGS = TERMS // 2
JUMPS = (1, -1, 3)
BF16 = jnp.bfloat16
F32 = jnp.float32
VMEM = pl.BlockSpec(memory_space=pltpu.VMEM)
SMEM = pl.BlockSpec(memory_space=pltpu.SMEM)


def partner(stage, term, sector):
    ring, half = term // 2, term % 2
    if stage == 3:
        return 2 * ring + 1 - half
    sign = 1 - 2 * ((ring + sector) % 2)
    return 2 * ((ring + sign * JUMPS[stage] + RINGS) % RINGS) + half


def swap(block, where):
    route = []
    for term in range(TERMS):
        for sector in range(SECTORS):
            other = where(term, sector)
            if other is not None:
                route.append((term * SECTORS + sector, other[0] * SECTORS + other[1]))
    return lax.ppermute(block, ("term", "sec"), route)


def pair_sector(term, sector):
    return term, sector ^ 1


def next_sector(term, sector):
    other = sector + 1 if sector % 2 else sector - 1
    return (term, other) if 0 <= other < SECTORS else None


def stage_route(stage):
    return lambda term, sector: (partner(stage, term, sector), sector)


def far_route(term, sector):
    return partner(3, partner(2, term, sector), sector), sector


def sizes_here(sizes_ref, shift_ref):
    sector = lax.axis_index("sec")
    source = sector + shift_ref[0]
    inside = (source >= 0) & (source < SECTORS)
    source_size = jnp.where(inside, sizes_ref[jnp.clip(source, 0, SECTORS - 1)], 0)
    return sizes_ref[sector], source_size


def ones_below(size, start, count, dim):
    shape = (count, 1) if dim == 0 else (1, count)
    index = lax.broadcasted_iota(jnp.int32, shape, dim) + start
    return jnp.where(index < size, 1.0, 0.0).astype(BF16)


def piece_at(slot):
    term, sector = lax.axis_index("term"), lax.axis_index("sec")
    for stage in range(4):
        if not (slot >> (3 - stage)) & 1:
            term = partner(stage, term, sector)
    return term


def prepare_kernel(sizes_ref, shift_ref, left_ref, right_ref, site_ref, left_out, right_out, site_out):
    own, source = sizes_here(sizes_ref, shift_ref)
    own_columns = ones_below(own, 0, WIDTH, 1)
    source_columns = ones_below(source, 0, WIDTH, 1)
    for slot in range(TERMS):
        start = pl.multiple_of(piece_at(slot) * PIECE, 16)
        here = pl.ds(slot * PIECE, PIECE)
        rows = ones_below(own, start, PIECE, 0)
        left_out[here, :] = left_ref[pl.ds(start, PIECE), :] * rows * source_columns
        site_out[here, :] = site_ref[pl.ds(start, PIECE), :] * own_columns
        source_rows = ones_below(source, slot * PIECE, PIECE, 0)
        right_out[here, :] = right_ref[here, :] * source_rows * own_columns


def chosen(shift_ref, own_ref, pair_ref, next_ref):
    shift = shift_ref[0]
    even = lax.axis_index("sec") % 2 == 0
    from_pair = jnp.where(even, shift == 1, shift == -1)
    return jnp.where(shift == 0, own_ref[...], jnp.where(from_pair, pair_ref[...], next_ref[...]))


def apply_kernel(chunk, shift_ref, own_ref, pair_ref, next_ref, right_ref, left_ref, send_ref, keep_ref):
    source = chosen(shift_ref, own_ref, pair_ref, next_ref)
    columns = pl.ds(chunk * SPAN, SPAN)
    mixed = jnp.dot(source, right_ref[:, columns], preferred_element_type=F32).astype(BF16)
    half = WIDTH // 2
    send_ref[...] = jnp.dot(left_ref[:half, :], mixed, preferred_element_type=F32).astype(BF16)
    keep_ref[...] = jnp.dot(left_ref[half:, :], mixed, preferred_element_type=F32)


def first_merge_kernel(*refs):
    send_out, keep_out = refs[-2:]
    half = WIDTH // 4
    for chunk in range(CHUNKS):
        keep, got = refs[2 * chunk : 2 * chunk + 2]
        columns = pl.ds(chunk * SPAN, SPAN)
        send_out[:, columns] = (keep[:half, :] + got[:half, :].astype(F32)).astype(BF16)
        keep_out[:, columns] = keep[half:, :] + got[half:, :].astype(F32)


def second_merge_kernel(keep_ref, got_ref, far_out, ring_out, half_out, keep_out):
    for slot, out in enumerate((far_out, ring_out, half_out, keep_out)):
        here = pl.ds(slot * PIECE, PIECE)
        out[...] = (keep_ref[here, :] + got_ref[here, :].astype(F32)).astype(out.dtype)


def finish_kernel(keep_ref, far_ref, ring_ref, half_ref, done_ref, out_ref):
    del done_ref
    total = keep_ref[...] + half_ref[...].astype(F32)
    out_ref[...] = total + (ring_ref[...].astype(F32) + far_ref[...].astype(F32))


def carry_kernel(shift_ref, own_ref, pair_ref, next_ref, left_ref, after_ref, out_ref):
    del after_ref
    source = chosen(shift_ref, own_ref, pair_ref, next_ref)
    out_ref[...] = jnp.dot(left_ref[...], source, preferred_element_type=F32).astype(BF16)


def renew_kernel(sizes_ref, shift_ref, carried_ref, site_ref, after_ref, out_ref, done_ref):
    del after_ref
    done_ref[...] = jnp.zeros(done_ref.shape, F32)
    _, source_size = sizes_here(sizes_ref, shift_ref)
    carried = carried_ref[...] * ones_below(source_size, 0, WIDTH, 1)
    renewed = lax.dot_general(
        site_ref[...], carried, (((0,), (0,)), ((), ())), preferred_element_type=F32
    )
    out_ref[...] = renewed.astype(BF16)


def room(mebibytes):
    return pltpu.CompilerParams(vmem_limit_bytes=mebibytes * 1024 * 1024)


def cost(flops, moved):
    return pl.CostEstimate(flops=flops, bytes_accessed=moved, transcendentals=0)


def shards(state, left_environment, right_environment, site_blocks, sector_sizes, term_shift):
    square = jax.ShapeDtypeStruct((WIDTH, WIDTH), BF16)
    state_own, site_own = state[0], site_blocks[0]
    state_next = swap(state_own, next_sector)
    state_pair = swap(state_own, pair_sector)
    site_next = swap(site_own, next_sector)
    site_pair = swap(site_own, pair_sector)
    left, right, site = pl.pallas_call(
        prepare_kernel,
        out_shape=(square, square, square),
        in_specs=[SMEM, SMEM, VMEM, VMEM, VMEM],
        out_specs=(VMEM, VMEM, VMEM),
        cost_estimate=cost(6_000_000, 7_000_000),
        compiler_params=room(20),
        name="prepare",
    )(sector_sizes, term_shift, left_environment[0, 0], right_environment[0, 0], site_own)
    flow = []
    for chunk in range(CHUNKS):
        half = WIDTH // 2
        flow.append(
            pl.pallas_call(
                functools.partial(apply_kernel, chunk),
                out_shape=(
                    jax.ShapeDtypeStruct((half, SPAN), BF16),
                    jax.ShapeDtypeStruct((half, SPAN), F32),
                ),
                in_specs=[SMEM] + [VMEM] * 5,
                out_specs=(VMEM, VMEM),
                cost_estimate=cost(4 * WIDTH * WIDTH * SPAN, 6_000_000),
                compiler_params=room(20),
        name="apply",
            )(term_shift, state_own, state_pair, state_next, right, left)
        )
    arrived = []
    for send, keep in flow:
        arrived += [keep, swap(send, stage_route(0))]
    quarter = WIDTH // 4
    send, keep = pl.pallas_call(
        first_merge_kernel,
        out_shape=(
            jax.ShapeDtypeStruct((quarter, WIDTH), BF16),
            jax.ShapeDtypeStruct((quarter, WIDTH), F32),
        ),
        in_specs=[VMEM] * (2 * CHUNKS),
        out_specs=(VMEM, VMEM),
        compiler_params=room(6),
        cost_estimate=cost(2 * quarter * WIDTH, 8 * quarter * WIDTH),
        name="first_merge",
    )(*arrived)
    got = swap(send, stage_route(1))
    carried = pl.pallas_call(
        carry_kernel,
        out_shape=square,
        in_specs=[SMEM] + [VMEM] * 4 + [pl.BlockSpec(memory_space=pl.ANY)],
        out_specs=VMEM,
        compiler_params=room(12),
        cost_estimate=cost(2 * WIDTH * WIDTH * WIDTH, 5_000_000),
        name="carry",
    )(term_shift, site_own, site_pair, site_next, left, send)
    piece = jax.ShapeDtypeStruct((PIECE, WIDTH), BF16)
    far, ring, half, keep = pl.pallas_call(
        second_merge_kernel,
        out_shape=(piece, piece, piece, jax.ShapeDtypeStruct((PIECE, WIDTH), F32)),
        in_specs=[VMEM, VMEM],
        out_specs=(VMEM,) * 4,
        compiler_params=room(6),
        cost_estimate=cost(quarter * WIDTH, 8 * quarter * WIDTH),
        name="second_merge",
    )(keep, got)
    far_got = swap(far, far_route)
    ring_got = swap(ring, stage_route(2))
    half_got = swap(half, stage_route(3))
    renewed, done = pl.pallas_call(
        renew_kernel,
        out_shape=(square, jax.ShapeDtypeStruct((8, 128), F32)),
        in_specs=[SMEM, SMEM, VMEM, VMEM, pl.BlockSpec(memory_space=pl.ANY)],
        out_specs=(VMEM, VMEM),
        compiler_params=room(12),
        cost_estimate=cost(2 * WIDTH * WIDTH * WIDTH, 4_000_000),
        name="renew",
    )(sector_sizes, term_shift, carried, site, keep)
    applied = pl.pallas_call(
        finish_kernel,
        out_shape=jax.ShapeDtypeStruct((PIECE, WIDTH), F32),
        in_specs=[VMEM] * 4 + [pl.BlockSpec(memory_space=pl.ANY)],
        out_specs=VMEM,
        compiler_params=room(4),
        cost_estimate=cost(4 * PIECE * WIDTH, 8 * PIECE * WIDTH),
        name="finish",
    )(keep, far_got, ring_got, half_got, done)
    return applied[None], renewed[None, None]


def solution(mesh):
    placed = (
        P("sec", None, None),
        P("term", "sec", None, None),
        P("term", "sec", None, None),
        P("sec", None, None),
        P(),
        P("term"),
    )
    return jax.shard_map(
        shards,
        mesh=mesh,
        in_specs=placed,
        out_specs=(P("sec", "term", None), P("term", "sec", None, None)),
        check_vma=False,
    )
```

```python
import functools

import jax
import jax.numpy as jnp
from jax import lax
from jax.experimental import pallas as pl
from jax.experimental.pallas import tpu as pltpu
from jax.sharding import PartitionSpec as P


WIDTH = 768
TERMS = 16
SECTORS = 16
PIECE = WIDTH // TERMS
CHUNKS = 2
SPAN = WIDTH // CHUNKS
RINGS = TERMS // 2
JUMPS = (1, -1, 3)
BF16 = jnp.bfloat16
F32 = jnp.float32
VMEM = pl.BlockSpec(memory_space=pltpu.VMEM)
SMEM = pl.BlockSpec(memory_space=pltpu.SMEM)


def partner(stage, term, sector):
    ring, half = term // 2, term % 2
    if stage == 3:
        return 2 * ring + 1 - half
    sign = 1 - 2 * ((ring + sector) % 2)
    return 2 * ((ring + sign * JUMPS[stage] + RINGS) % RINGS) + half


def swap(block, where):
    route = []
    for term in range(TERMS):
        for sector in range(SECTORS):
            other_term, other_sector = where(term, sector)
            route.append((term * SECTORS + sector, other_term * SECTORS + other_sector))
    return lax.ppermute(block, ("term", "sec"), route)


def pair_sector(term, sector):
    return term, sector ^ 1


def next_sector(term, sector):
    return term, (sector + 1 if sector % 2 else sector - 1) % SECTORS


def stage_route(stage):
    return lambda term, sector: (partner(stage, term, sector), sector)


def far_route(term, sector):
    return partner(3, partner(2, term, sector), sector), sector


def sizes_here(sizes_ref, shift_ref):
    sector = lax.axis_index("sec")
    source = sector + shift_ref[0]
    inside = (source >= 0) & (source < SECTORS)
    source_size = jnp.where(inside, sizes_ref[jnp.clip(source, 0, SECTORS - 1)], 0)
    return sizes_ref[sector], source_size


def ones_below(size, start, count, dim):
    shape = (count, 1) if dim == 0 else (1, count)
    index = lax.broadcasted_iota(jnp.int32, shape, dim) + start
    return jnp.where(index < size, 1.0, 0.0).astype(BF16)


def piece_at(slot):
    term, sector = lax.axis_index("term"), lax.axis_index("sec")
    for stage in range(4):
        if not (slot >> (3 - stage)) & 1:
            term = partner(stage, term, sector)
    return term


def prepare_kernel(sizes_ref, shift_ref, left_ref, right_ref, site_ref, left_out, right_out, site_out):
    own, source = sizes_here(sizes_ref, shift_ref)
    own_columns = ones_below(own, 0, WIDTH, 1)
    source_columns = ones_below(source, 0, WIDTH, 1)
    for slot in range(TERMS):
        start = pl.multiple_of(piece_at(slot) * PIECE, 16)
        here = pl.ds(slot * PIECE, PIECE)
        rows = ones_below(own, start, PIECE, 0)
        left_out[here, :] = left_ref[pl.ds(start, PIECE), :] * rows * source_columns
        site_out[here, :] = site_ref[pl.ds(start, PIECE), :] * own_columns
        source_rows = ones_below(source, slot * PIECE, PIECE, 0)
        right_out[here, :] = right_ref[here, :] * source_rows * own_columns


def chosen(shift_ref, own_ref, pair_ref, next_ref):
    shift = shift_ref[0]
    even = lax.axis_index("sec") % 2 == 0
    from_pair = jnp.where(even, shift == 1, shift == -1)
    return jnp.where(shift == 0, own_ref[...], jnp.where(from_pair, pair_ref[...], next_ref[...]))


def apply_kernel(chunk, shift_ref, own_ref, pair_ref, next_ref, right_ref, left_ref, send_ref, keep_ref):
    source = chosen(shift_ref, own_ref, pair_ref, next_ref)
    columns = pl.ds(chunk * SPAN, SPAN)
    mixed = jnp.dot(source, right_ref[:, columns], preferred_element_type=F32).astype(BF16)
    half = WIDTH // 2
    send_ref[...] = jnp.dot(left_ref[:half, :], mixed, preferred_element_type=F32).astype(BF16)
    keep_ref[...] = jnp.dot(left_ref[half:, :], mixed, preferred_element_type=F32)


def first_merge_kernel(keep_ref, got_ref, send_out, keep_out):
    half = keep_ref.shape[0] // 2
    send_out[...] = (keep_ref[:half, :] + got_ref[:half, :].astype(F32)).astype(BF16)
    keep_out[...] = keep_ref[half:, :] + got_ref[half:, :].astype(F32)


def second_merge_kernel(*refs):
    outs = refs[2 * CHUNKS :]
    for chunk in range(CHUNKS):
        keep, got = refs[2 * chunk : 2 * chunk + 2]
        columns = pl.ds(chunk * SPAN, SPAN)
        for slot, out in enumerate(outs):
            here = pl.ds(slot * PIECE, PIECE)
            out[:, columns] = (keep[here, :] + got[here, :].astype(F32)).astype(out.dtype)


def finish_kernel(keep_ref, far_ref, ring_ref, half_ref, done_ref, out_ref):
    del done_ref
    total = keep_ref[...] + half_ref[...].astype(F32)
    out_ref[...] = total + (ring_ref[...].astype(F32) + far_ref[...].astype(F32))


def carry_kernel(shift_ref, own_ref, pair_ref, next_ref, left_ref, after_ref, out_ref):
    del after_ref
    source = chosen(shift_ref, own_ref, pair_ref, next_ref)
    out_ref[...] = jnp.dot(left_ref[...], source, preferred_element_type=F32).astype(BF16)


def renew_kernel(sizes_ref, shift_ref, carried_ref, site_ref, after_ref, out_ref, done_ref):
    del after_ref
    done_ref[...] = jnp.zeros(done_ref.shape, F32)
    _, source_size = sizes_here(sizes_ref, shift_ref)
    carried = carried_ref[...] * ones_below(source_size, 0, WIDTH, 1)
    renewed = lax.dot_general(
        site_ref[...], carried, (((0,), (0,)), ((), ())), preferred_element_type=F32
    )
    out_ref[...] = renewed.astype(BF16)


def room(mebibytes):
    return pltpu.CompilerParams(vmem_limit_bytes=mebibytes * 1024 * 1024)


def cost(flops, moved):
    return pl.CostEstimate(flops=flops, bytes_accessed=moved, transcendentals=0)


def shards(state, left_environment, right_environment, site_blocks, sector_sizes, term_shift):
    square = jax.ShapeDtypeStruct((WIDTH, WIDTH), BF16)
    state_own, site_own = state[0], site_blocks[0]
    state_next = swap(state_own, next_sector)
    state_pair = swap(state_own, pair_sector)
    site_next = swap(site_own, next_sector)
    site_pair = swap(site_own, pair_sector)
    left, right, site = pl.pallas_call(
        prepare_kernel,
        out_shape=(square, square, square),
        in_specs=[SMEM, SMEM, VMEM, VMEM, VMEM],
        out_specs=(VMEM, VMEM, VMEM),
        cost_estimate=cost(6_000_000, 7_000_000),
        compiler_params=room(20),
        name="prepare",
    )(sector_sizes, term_shift, left_environment[0, 0], right_environment[0, 0], site_own)
    flow = []
    for chunk in range(CHUNKS):
        half = WIDTH // 2
        flow.append(
            pl.pallas_call(
                functools.partial(apply_kernel, chunk),
                out_shape=(
                    jax.ShapeDtypeStruct((half, SPAN), BF16),
                    jax.ShapeDtypeStruct((half, SPAN), F32),
                ),
                in_specs=[SMEM] + [VMEM] * 5,
                out_specs=(VMEM, VMEM),
                cost_estimate=cost(4 * WIDTH * WIDTH * SPAN, 6_000_000),
                compiler_params=room(20),
        name="apply",
            )(term_shift, state_own, state_pair, state_next, right, left)
        )
    quarter = WIDTH // 4
    arrived = [(keep, swap(send, stage_route(0))) for send, keep in flow]
    flow = []
    for keep, got in arrived:
        flow.append(
            pl.pallas_call(
                first_merge_kernel,
                out_shape=(
                    jax.ShapeDtypeStruct((quarter, SPAN), BF16),
                    jax.ShapeDtypeStruct((quarter, SPAN), F32),
                ),
                in_specs=[VMEM, VMEM],
                out_specs=(VMEM, VMEM),
                compiler_params=room(6),
                cost_estimate=cost(2 * quarter * SPAN, 8 * quarter * SPAN),
                name="first_merge",
            )(keep, got)
        )
    arrived = []
    for send, keep in flow:
        arrived += [keep, swap(send, stage_route(1))]
    carried = pl.pallas_call(
        carry_kernel,
        out_shape=square,
        in_specs=[SMEM] + [VMEM] * 4 + [pl.BlockSpec(memory_space=pl.ANY)],
        out_specs=VMEM,
        compiler_params=room(12),
        cost_estimate=cost(2 * WIDTH * WIDTH * WIDTH, 5_000_000),
        name="carry",
    )(term_shift, site_own, site_pair, site_next, left, flow[-1][0])
    piece = jax.ShapeDtypeStruct((PIECE, WIDTH), BF16)
    far, ring, half, keep = pl.pallas_call(
        second_merge_kernel,
        out_shape=(piece, piece, piece, jax.ShapeDtypeStruct((PIECE, WIDTH), F32)),
        in_specs=[VMEM] * (2 * CHUNKS),
        out_specs=(VMEM,) * 4,
        compiler_params=room(6),
        cost_estimate=cost(quarter * WIDTH, 8 * quarter * WIDTH),
        name="second_merge",
    )(*arrived)
    far_got = swap(far, far_route)
    ring_got = swap(ring, stage_route(2))
    half_got = swap(half, stage_route(3))
    renewed, done = pl.pallas_call(
        renew_kernel,
        out_shape=(square, jax.ShapeDtypeStruct((8, 128), F32)),
        in_specs=[SMEM, SMEM, VMEM, VMEM, pl.BlockSpec(memory_space=pl.ANY)],
        out_specs=(VMEM, VMEM),
        compiler_params=room(12),
        cost_estimate=cost(2 * WIDTH * WIDTH * WIDTH, 4_000_000),
        name="renew",
    )(sector_sizes, term_shift, carried, site, keep)
    applied = pl.pallas_call(
        finish_kernel,
        out_shape=jax.ShapeDtypeStruct((PIECE, WIDTH), F32),
        in_specs=[VMEM] * 4 + [pl.BlockSpec(memory_space=pl.ANY)],
        out_specs=VMEM,
        compiler_params=room(4),
        cost_estimate=cost(4 * PIECE * WIDTH, 8 * PIECE * WIDTH),
        name="finish",
    )(keep, far_got, ring_got, half_got, done)
    return applied[None], renewed[None, None]


def solution(mesh):
    placed = (
        P("sec", None, None),
        P("term", "sec", None, None),
        P("term", "sec", None, None),
        P("sec", None, None),
        P(),
        P("term"),
    )
    return jax.shard_map(
        shards,
        mesh=mesh,
        in_specs=placed,
        out_specs=(P("sec", "term", None), P("term", "sec", None, None)),
        check_vma=False,
    )
```

```python
import functools

import jax
import jax.numpy as jnp
from jax import lax
from jax.experimental import pallas as pl
from jax.experimental.pallas import tpu as pltpu
from jax.sharding import PartitionSpec as P


WIDTH = 768
TERMS = 16
SECTORS = 16
PIECE = WIDTH // TERMS
QUARTER = WIDTH // 4
RINGS = TERMS // 2
JUMPS = (1, -1, 3)
BF16 = jnp.bfloat16
F32 = jnp.float32
VMEM = pl.BlockSpec(memory_space=pltpu.VMEM)
SMEM = pl.BlockSpec(memory_space=pltpu.SMEM)


def partner(stage, term, sector):
    ring, half = term // 2, term % 2
    if stage == 3:
        return 2 * ring + 1 - half
    sign = 1 - 2 * ((ring + sector) % 2)
    return 2 * ((ring + sign * JUMPS[stage] + RINGS) % RINGS) + half


def swap(block, where):
    route = []
    for term in range(TERMS):
        for sector in range(SECTORS):
            other_term, other_sector = where(term, sector)
            route.append((term * SECTORS + sector, other_term * SECTORS + other_sector))
    return lax.ppermute(block, ("term", "sec"), route)


def pair_sector(term, sector):
    return term, sector ^ 1


def next_sector(term, sector):
    return term, (sector + 1 if sector % 2 else sector - 1) % SECTORS


def stage_route(stage):
    return lambda term, sector: (partner(stage, term, sector), sector)


def far_route(term, sector):
    return partner(3, partner(2, term, sector), sector), sector


def sizes_here(sizes_ref, shift_ref):
    sector = lax.axis_index("sec")
    source = sector + shift_ref[0]
    inside = (source >= 0) & (source < SECTORS)
    source_size = jnp.where(inside, sizes_ref[jnp.clip(source, 0, SECTORS - 1)], 0)
    return sizes_ref[sector], source_size


def ones_below(size, start, count, dim):
    shape = (count, 1) if dim == 0 else (1, count)
    index = lax.broadcasted_iota(jnp.int32, shape, dim) + start
    return jnp.where(index < size, 1.0, 0.0).astype(BF16)


def piece_at(slot):
    term, sector = lax.axis_index("term"), lax.axis_index("sec")
    for stage in range(4):
        if not (slot >> (3 - stage)) & 1:
            term = partner(stage, term, sector)
    return term


def prepare_kernel(sizes_ref, shift_ref, left_ref, right_ref, site_ref, left_out, right_out, site_out):
    own, source = sizes_here(sizes_ref, shift_ref)
    own_columns = ones_below(own, 0, WIDTH, 1)
    source_columns = ones_below(source, 0, WIDTH, 1)
    for slot in range(TERMS):
        start = pl.multiple_of(piece_at(slot) * PIECE, 16)
        here = pl.ds(slot * PIECE, PIECE)
        rows = ones_below(own, start, PIECE, 0)
        left_out[here, :] = left_ref[pl.ds(start, PIECE), :] * rows * source_columns
        site_out[here, :] = site_ref[pl.ds(start, PIECE), :] * own_columns
        source_rows = ones_below(source, slot * PIECE, PIECE, 0)
        right_out[here, :] = right_ref[here, :] * source_rows * own_columns


def with_source(shift_ref, own_ref, pair_ref, next_ref, body):
    shift = shift_ref[0]
    even = lax.axis_index("sec") % 2 == 0
    local = shift == 0
    from_pair = (shift == 1) == even

    @pl.when(local)
    def _():
        body(own_ref)

    @pl.when(jnp.logical_not(local) & from_pair)
    def _():
        body(pair_ref)

    @pl.when(jnp.logical_not(local) & jnp.logical_not(from_pair))
    def _():
        body(next_ref)


def mix_kernel(shift_ref, own_ref, pair_ref, next_ref, right_ref, left_ref, mixed_out, send_out):
    def body(source_ref):
        mixed = jnp.dot(source_ref[...], right_ref[...], preferred_element_type=F32).astype(BF16)
        mixed_out[...] = mixed
        send_out[...] = jnp.dot(left_ref[:QUARTER, :], mixed, preferred_element_type=F32).astype(BF16)

    with_source(shift_ref, own_ref, pair_ref, next_ref, body)


def send_kernel(left_ref, mixed_ref, send_out):
    rows = left_ref[QUARTER : 2 * QUARTER, :]
    send_out[...] = jnp.dot(rows, mixed_ref[...], preferred_element_type=F32).astype(BF16)


def keep_kernel(left_ref, mixed_ref, after_ref, first_out, second_out):
    del after_ref
    for part, out in ((2, first_out), (3, second_out)):
        rows = left_ref[part * QUARTER : (part + 1) * QUARTER, :]
        out[...] = jnp.dot(rows, mixed_ref[...], preferred_element_type=F32)


def pass_kernel(keep_ref, got_ref, first_out, second_out):
    for here, out in ((pl.ds(0, PIECE), first_out), (pl.ds(PIECE, 3 * PIECE), second_out)):
        out[...] = (keep_ref[here, :] + got_ref[here, :].astype(F32)).astype(BF16)


def hold_kernel(keep_ref, got_ref, out_ref):
    out_ref[...] = keep_ref[...] + got_ref[...].astype(F32)


def split_kernel(start, hold_ref, got_ref, *outs):
    for slot, out in enumerate(outs):
        mine, theirs = pl.ds((start + slot) * PIECE, PIECE), pl.ds(slot * PIECE, PIECE)
        out[...] = (hold_ref[mine, :] + got_ref[theirs, :].astype(F32)).astype(out.dtype)


def finish_kernel(keep_ref, far_ref, ring_ref, half_ref, done_ref, out_ref):
    del done_ref
    total = keep_ref[...] + half_ref[...].astype(F32)
    out_ref[...] = total + (ring_ref[...].astype(F32) + far_ref[...].astype(F32))


def carry_kernel(shift_ref, own_ref, pair_ref, next_ref, left_ref, after_ref, out_ref):
    del after_ref

    def body(source_ref):
        carried = jnp.dot(left_ref[...], source_ref[...], preferred_element_type=F32)
        out_ref[...] = carried.astype(BF16)

    with_source(shift_ref, own_ref, pair_ref, next_ref, body)


def renew_kernel(sizes_ref, shift_ref, carried_ref, site_ref, after_ref, out_ref, done_ref):
    del after_ref
    done_ref[...] = jnp.zeros(done_ref.shape, F32)
    _, source_size = sizes_here(sizes_ref, shift_ref)
    carried = carried_ref[...] * ones_below(source_size, 0, WIDTH, 1)
    renewed = lax.dot_general(
        site_ref[...], carried, (((0,), (0,)), ((), ())), preferred_element_type=F32
    )
    out_ref[...] = renewed.astype(BF16)


def room(mebibytes):
    return pltpu.CompilerParams(vmem_limit_bytes=mebibytes * 1024 * 1024)


def cost(flops, moved):
    return pl.CostEstimate(flops=flops, bytes_accessed=moved, transcendentals=0)


def shards(state, left_environment, right_environment, site_blocks, sector_sizes, term_shift):
    square = jax.ShapeDtypeStruct((WIDTH, WIDTH), BF16)
    state_own, site_own = state[0], site_blocks[0]
    state_next = swap(state_own, next_sector)
    state_pair = swap(state_own, pair_sector)
    site_next = swap(site_own, next_sector)
    site_pair = swap(site_own, pair_sector)
    left, right, site = pl.pallas_call(
        prepare_kernel,
        out_shape=(square, square, square),
        in_specs=[SMEM, SMEM, VMEM, VMEM, VMEM],
        out_specs=(VMEM, VMEM, VMEM),
        cost_estimate=cost(6_000_000, 7_000_000),
        compiler_params=room(20),
        name="prepare",
    )(sector_sizes, term_shift, left_environment[0, 0], right_environment[0, 0], site_own)
    anywhere = pl.BlockSpec(memory_space=pl.ANY)
    strip = jax.ShapeDtypeStruct((QUARTER, WIDTH), BF16)
    strip_sum = jax.ShapeDtypeStruct((QUARTER, WIDTH), F32)
    strip_flops = 2 * QUARTER * WIDTH * WIDTH
    mixed, send_first = pl.pallas_call(
        mix_kernel,
        out_shape=(square, strip),
        in_specs=[SMEM] + [VMEM] * 5,
        out_specs=(VMEM, VMEM),
        compiler_params=room(20),
        cost_estimate=cost(5 * strip_flops, 6_000_000),
        name="mix",
    )(term_shift, state_own, state_pair, state_next, right, left)
    got_first = swap(send_first, stage_route(0))
    send_second = pl.pallas_call(
        send_kernel,
        out_shape=strip,
        in_specs=[VMEM, VMEM],
        out_specs=VMEM,
        compiler_params=room(12),
        cost_estimate=cost(strip_flops, 2_000_000),
        name="send",
    )(left, mixed)
    got_second = swap(send_second, stage_route(0))
    keep_first, keep_second = pl.pallas_call(
        keep_kernel,
        out_shape=(strip_sum, strip_sum),
        in_specs=[VMEM, VMEM, anywhere],
        out_specs=(VMEM, VMEM),
        compiler_params=room(12),
        cost_estimate=cost(2 * strip_flops, 3_000_000),
        name="keep",
    )(left, mixed, send_second)
    piece = jax.ShapeDtypeStruct((PIECE, WIDTH), BF16)
    pieces = jax.ShapeDtypeStruct((3 * PIECE, WIDTH), BF16)
    pass_first, pass_second = pl.pallas_call(
        pass_kernel,
        out_shape=(piece, pieces),
        in_specs=[VMEM, VMEM],
        out_specs=(VMEM, VMEM),
        compiler_params=room(6),
        cost_estimate=cost(QUARTER * WIDTH, 8 * QUARTER * WIDTH),
        name="pass",
    )(keep_first, got_first)
    moved_first = swap(pass_first, stage_route(1))
    moved_second = swap(pass_second, stage_route(1))
    held = pl.pallas_call(
        hold_kernel,
        out_shape=strip_sum,
        in_specs=[VMEM, VMEM],
        out_specs=VMEM,
        compiler_params=room(6),
        cost_estimate=cost(QUARTER * WIDTH, 8 * QUARTER * WIDTH),
        name="hold",
    )(keep_second, got_second)
    carried = pl.pallas_call(
        carry_kernel,
        out_shape=square,
        in_specs=[SMEM] + [VMEM] * 4 + [anywhere],
        out_specs=VMEM,
        compiler_params=room(12),
        cost_estimate=cost(4 * strip_flops, 5_000_000),
        name="carry",
    )(term_shift, site_own, site_pair, site_next, left, held)
    (far,) = pl.pallas_call(
        functools.partial(split_kernel, 0),
        out_shape=(piece,),
        in_specs=[VMEM, VMEM],
        out_specs=(VMEM,),
        compiler_params=room(6),
        cost_estimate=cost(PIECE * WIDTH, 8 * PIECE * WIDTH),
        name="split_first",
    )(held, moved_first)
    far_got = swap(far, far_route)
    ring, half, keep = pl.pallas_call(
        functools.partial(split_kernel, 1),
        out_shape=(piece, piece, jax.ShapeDtypeStruct((PIECE, WIDTH), F32)),
        in_specs=[VMEM, VMEM],
        out_specs=(VMEM, VMEM, VMEM),
        compiler_params=room(6),
        cost_estimate=cost(3 * PIECE * WIDTH, 24 * PIECE * WIDTH),
        name="split_second",
    )(held, moved_second)
    ring_got = swap(ring, stage_route(2))
    half_got = swap(half, stage_route(3))
    renewed, done = pl.pallas_call(
        renew_kernel,
        out_shape=(square, jax.ShapeDtypeStruct((8, 128), F32)),
        in_specs=[SMEM, SMEM, VMEM, VMEM, pl.BlockSpec(memory_space=pl.ANY)],
        out_specs=(VMEM, VMEM),
        compiler_params=room(12),
        cost_estimate=cost(2 * WIDTH * WIDTH * WIDTH, 4_000_000),
        name="renew",
    )(sector_sizes, term_shift, carried, site, keep)
    applied = pl.pallas_call(
        finish_kernel,
        out_shape=jax.ShapeDtypeStruct((PIECE, WIDTH), F32),
        in_specs=[VMEM] * 4 + [pl.BlockSpec(memory_space=pl.ANY)],
        out_specs=VMEM,
        compiler_params=room(4),
        cost_estimate=cost(4 * PIECE * WIDTH, 8 * PIECE * WIDTH),
        name="finish",
    )(keep, far_got, ring_got, half_got, done)
    return applied[None], renewed[None, None]


def solution(mesh):
    placed = (
        P("sec", None, None),
        P("term", "sec", None, None),
        P("term", "sec", None, None),
        P("sec", None, None),
        P(),
        P("term"),
    )
    return jax.shard_map(
        shards,
        mesh=mesh,
        in_specs=placed,
        out_specs=(P("sec", "term", None), P("term", "sec", None, None)),
        check_vma=False,
    )
```

```python
import functools

import jax
import jax.numpy as jnp
from jax import lax
from jax.experimental import pallas as pl
from jax.experimental.pallas import tpu as pltpu
from jax.sharding import PartitionSpec as P


WIDTH = 768
TERMS = 16
SECTORS = 16
PIECE = WIDTH // TERMS
QUARTER = WIDTH // 4
RELAYED = 160
DIRECT = WIDTH - 2 * RELAYED
RINGS = TERMS // 2
JUMPS = (1, -1, 3)
BF16 = jnp.bfloat16
F32 = jnp.float32
VMEM = pl.BlockSpec(memory_space=pltpu.VMEM)
SMEM = pl.BlockSpec(memory_space=pltpu.SMEM)
HBM = pl.BlockSpec(memory_space=pltpu.HBM)


def partner(stage, term, sector):
    ring, half = term // 2, term % 2
    if stage == 3:
        return 2 * ring + 1 - half
    sign = 1 - 2 * ((ring + sector) % 2)
    return 2 * ((ring + sign * JUMPS[stage] + RINGS) % RINGS) + half


def swap(block, where):
    route = []
    for term in range(TERMS):
        for sector in range(SECTORS):
            other_term, other_sector = where(term, sector)
            route.append((term * SECTORS + sector, other_term * SECTORS + other_sector))
    return lax.ppermute(block, ("term", "sec"), route)


def pair_sector(term, sector):
    return term, sector ^ 1


def next_sector(term, sector):
    return term, (sector + 1 if sector % 2 else sector - 1) % SECTORS


def stage_route(stage):
    return lambda term, sector: (partner(stage, term, sector), sector)


def far_route(term, sector):
    return partner(3, partner(2, term, sector), sector), sector


def sizes_here(sizes_ref, shift_ref):
    sector = lax.axis_index("sec")
    source = sector + shift_ref[0]
    inside = (source >= 0) & (source < SECTORS)
    source_size = jnp.where(inside, sizes_ref[jnp.clip(source, 0, SECTORS - 1)], 0)
    return sizes_ref[sector], source_size


def ones_below(size, start, count, dim):
    shape = (count, 1) if dim == 0 else (1, count)
    index = lax.broadcasted_iota(jnp.int32, shape, dim) + start
    return jnp.where(index < size, 1.0, 0.0).astype(BF16)


def piece_at(slot):
    term, sector = lax.axis_index("term"), lax.axis_index("sec")
    for stage in range(4):
        if not (slot >> (3 - stage)) & 1:
            term = partner(stage, term, sector)
    return term


def relay_starts():
    odd = (lax.axis_index("term") // 2 + lax.axis_index("sec")) % 2
    taken = DIRECT + RELAYED * odd
    passed = DIRECT + RELAYED * (1 - odd)
    return pl.multiple_of(taken, 16), pl.multiple_of(passed, 16)


def cut_kernel(state_ref, shared_out, direct_out, sems):
    others = relay_starts()[1]
    shared = pltpu.make_async_copy(state_ref.at[pl.ds(others, RELAYED), :], shared_out, sems.at[0])
    direct = pltpu.make_async_copy(state_ref.at[pl.ds(0, DIRECT), :], direct_out, sems.at[1])
    shared.start()
    direct.start()
    shared.wait()
    direct.wait()


def bring_kernel(state_ref, site_ref, out_ref, turned_out, sem):
    copy = pltpu.make_async_copy(state_ref, out_ref, sem)
    copy.start()
    turned_out[...] = site_ref[...].T
    copy.wait()


def prepare_kernel(
    sizes_ref,
    shift_ref,
    left_hbm,
    right_hbm,
    site_hbm,
    left_out,
    right_out,
    site_out,
    left_ref,
    right_ref,
    site_ref,
    sems,
):
    moves = ((left_hbm, left_ref), (right_hbm, right_ref), (site_hbm, site_ref))
    copies = [
        pltpu.make_async_copy(source, target, sems.at[index])
        for index, (source, target) in enumerate(moves)
    ]
    for copy in copies:
        copy.start()
    own, source = sizes_here(sizes_ref, shift_ref)
    own_columns = ones_below(own, 0, WIDTH, 1)
    source_columns = ones_below(source, 0, WIDTH, 1)
    for copy in copies:
        copy.wait()
    for slot in range(TERMS):
        start = pl.multiple_of(piece_at(slot) * PIECE, 16)
        here = pl.ds(slot * PIECE, PIECE)
        rows = ones_below(own, start, PIECE, 0)
        left_out[here, :] = left_ref[pl.ds(start, PIECE), :] * rows * source_columns
        site_out[here, :] = site_ref[pl.ds(start, PIECE), :] * own_columns
        source_rows = ones_below(source, slot * PIECE, PIECE, 0)
        right_out[here, :] = right_ref[here, :] * source_rows * own_columns


def with_source(shift_ref, own, pair, far):
    shift = shift_ref[0]
    even = lax.axis_index("sec") % 2 == 0
    local = shift == 0
    from_pair = (shift == 1) == even

    pl.when(local)(own)
    pl.when(jnp.logical_not(local) & from_pair)(pair)
    pl.when(jnp.logical_not(local) & jnp.logical_not(from_pair))(far)


def mix_kernel(
    shift_ref,
    own_ref,
    pair_ref,
    direct_ref,
    taken_ref,
    passed_ref,
    right_ref,
    left_ref,
    mixed_out,
    send_out,
    joined_ref,
):
    def body(source_ref):
        mixed = jnp.dot(source_ref[...], right_ref[...], preferred_element_type=F32).astype(BF16)
        mixed_out[...] = mixed
        send_out[...] = jnp.dot(left_ref[:QUARTER, :], mixed, preferred_element_type=F32).astype(BF16)

    def joined():
        taken, passed = relay_starts()
        joined_ref[:DIRECT, :] = direct_ref[...]
        joined_ref[pl.ds(taken, RELAYED), :] = taken_ref[...]
        joined_ref[pl.ds(passed, RELAYED), :] = passed_ref[...]
        body(joined_ref)

    with_source(shift_ref, lambda: body(own_ref), lambda: body(pair_ref), joined)


def send_kernel(left_ref, mixed_ref, send_out):
    rows = left_ref[QUARTER : 2 * QUARTER, :]
    send_out[...] = jnp.dot(rows, mixed_ref[...], preferred_element_type=F32).astype(BF16)


def keep_kernel(left_ref, mixed_ref, after_ref, first_out, second_out):
    del after_ref
    for part, out in ((2, first_out), (3, second_out)):
        rows = left_ref[part * QUARTER : (part + 1) * QUARTER, :]
        out[...] = jnp.dot(rows, mixed_ref[...], preferred_element_type=F32)


def pass_kernel(keep_ref, got_ref, first_out, second_out):
    for here, out in ((pl.ds(0, PIECE), first_out), (pl.ds(PIECE, 3 * PIECE), second_out)):
        out[...] = (keep_ref[here, :] + got_ref[here, :].astype(F32)).astype(BF16)


def hold_kernel(keep_ref, got_ref, out_ref):
    out_ref[...] = keep_ref[...] + got_ref[...].astype(F32)


def split_kernel(start, hold_ref, got_ref, *outs):
    for slot, out in enumerate(outs):
        mine, theirs = pl.ds((start + slot) * PIECE, PIECE), pl.ds(slot * PIECE, PIECE)
        out[...] = (hold_ref[mine, :] + got_ref[theirs, :].astype(F32)).astype(out.dtype)


def finish_kernel(keep_ref, far_ref, ring_ref, half_ref, done_ref, out_ref):
    del done_ref
    total = keep_ref[...] + half_ref[...].astype(F32)
    out_ref[...] = total + (ring_ref[...].astype(F32) + far_ref[...].astype(F32))


def carry_kernel(part, shift_ref, own_ref, pair_ref, next_ref, left_ref, after_ref, out_ref):
    del after_ref
    rows = pl.ds(part * 2 * QUARTER, 2 * QUARTER)

    def body(source_ref):
        carried = jnp.dot(left_ref[rows, :], source_ref[...], preferred_element_type=F32)
        out_ref[...] = carried.astype(BF16)

    with_source(shift_ref, *(functools.partial(body, ref) for ref in (own_ref, pair_ref, next_ref)))


def renew_kernel(
    sizes_ref, shift_ref, upper_ref, lower_ref, site_ref, after_ref, out_hbm, done_ref, rows_ref, sems
):
    del after_ref
    done_ref[...] = jnp.zeros(done_ref.shape, F32)
    _, source_size = sizes_here(sizes_ref, shift_ref)
    columns = ones_below(source_size, 0, WIDTH, 1)
    carried = jnp.concatenate([upper_ref[...] * columns, lower_ref[...] * columns], axis=0)
    copies = []
    for part in range(4):
        here = pl.ds(part * QUARTER, QUARTER)
        renewed = jnp.dot(site_ref[here, :], carried, preferred_element_type=F32)
        rows_ref[here, :] = renewed.astype(BF16)
        copies.append(
            pltpu.make_async_copy(rows_ref.at[here, :], out_hbm.at[here, :], sems.at[part])
        )
        copies[-1].start()
    for copy in copies:
        copy.wait()


def room(mebibytes):
    return pltpu.CompilerParams(vmem_limit_bytes=mebibytes * 1024 * 1024)


def cost(flops, moved):
    return pl.CostEstimate(flops=flops, bytes_accessed=moved, transcendentals=0)


def shards(state, left_environment, right_environment, site_blocks, sector_sizes, term_shift):
    square = jax.ShapeDtypeStruct((WIDTH, WIDTH), BF16)
    state_own, site_own = state[0], site_blocks[0]
    shared, direct = pl.pallas_call(
        cut_kernel,
        out_shape=(
            jax.ShapeDtypeStruct((RELAYED, WIDTH), BF16),
            jax.ShapeDtypeStruct((DIRECT, WIDTH), BF16),
        ),
        in_specs=[HBM],
        out_specs=(VMEM, VMEM),
        scratch_shapes=[pltpu.SemaphoreType.DMA((2,))],
        compiler_params=room(4),
        cost_estimate=cost(1000, 2_000_000),
        name="cut",
    )(state_own)
    taken = swap(shared, next_sector)
    direct_got = swap(direct, next_sector)
    state_pair = swap(state_own, pair_sector)
    passed = swap(taken, stage_route(0))
    site_next = swap(site_own, next_sector)
    site_pair = swap(site_own, pair_sector)
    left, right, site = pl.pallas_call(
        prepare_kernel,
        out_shape=(square,) * 3,
        in_specs=[SMEM, SMEM] + [HBM] * 3,
        out_specs=(VMEM,) * 3,
        scratch_shapes=[pltpu.VMEM((WIDTH, WIDTH), BF16)] * 3 + [pltpu.SemaphoreType.DMA((3,))],
        compiler_params=room(12),
        cost_estimate=cost(6_000_000, 1000),
        name="prepare",
    )(sector_sizes, term_shift, left_environment[0, 0], right_environment[0, 0], site_own)
    state_here, turned = pl.pallas_call(
        bring_kernel,
        out_shape=(square, square),
        in_specs=[HBM, VMEM],
        out_specs=(VMEM, VMEM),
        scratch_shapes=[pltpu.SemaphoreType.DMA],
        compiler_params=room(10),
        cost_estimate=cost(1000, 2_400_000),
        name="bring",
    )(state_own, site)
    anywhere = pl.BlockSpec(memory_space=pl.ANY)
    strip = jax.ShapeDtypeStruct((QUARTER, WIDTH), BF16)
    strip_sum = jax.ShapeDtypeStruct((QUARTER, WIDTH), F32)
    strip_flops = 2 * QUARTER * WIDTH * WIDTH
    mixed, send_first = pl.pallas_call(
        mix_kernel,
        out_shape=(square, strip),
        in_specs=[SMEM] + [VMEM] * 7,
        out_specs=(VMEM, VMEM),
        scratch_shapes=[pltpu.VMEM((WIDTH, WIDTH), BF16)],
        compiler_params=room(20),
        cost_estimate=cost(5 * strip_flops, 6_000_000),
        name="mix",
    )(term_shift, state_here, state_pair, direct_got, taken, passed, right, left)
    got_first = swap(send_first, stage_route(0))
    send_second = pl.pallas_call(
        send_kernel,
        out_shape=strip,
        in_specs=[VMEM, VMEM],
        out_specs=VMEM,
        compiler_params=room(12),
        cost_estimate=cost(strip_flops, 2_000_000),
        name="send",
    )(left, mixed)
    got_second = swap(send_second, stage_route(0))
    keep_first, keep_second = pl.pallas_call(
        keep_kernel,
        out_shape=(strip_sum, strip_sum),
        in_specs=[VMEM, VMEM, anywhere],
        out_specs=(VMEM, VMEM),
        compiler_params=room(12),
        cost_estimate=cost(2 * strip_flops, 3_000_000),
        name="keep",
    )(left, mixed, send_second)
    piece = jax.ShapeDtypeStruct((PIECE, WIDTH), BF16)
    pieces = jax.ShapeDtypeStruct((3 * PIECE, WIDTH), BF16)
    pass_first, pass_second = pl.pallas_call(
        pass_kernel,
        out_shape=(piece, pieces),
        in_specs=[VMEM, VMEM],
        out_specs=(VMEM, VMEM),
        compiler_params=room(6),
        cost_estimate=cost(QUARTER * WIDTH, 8 * QUARTER * WIDTH),
        name="pass",
    )(keep_first, got_first)
    moved_first = swap(pass_first, stage_route(1))
    moved_second = swap(pass_second, stage_route(1))
    held = pl.pallas_call(
        hold_kernel,
        out_shape=strip_sum,
        in_specs=[VMEM, VMEM],
        out_specs=VMEM,
        compiler_params=room(6),
        cost_estimate=cost(QUARTER * WIDTH, 8 * QUARTER * WIDTH),
        name="hold",
    )(keep_second, got_second)

    def carry(part, after):
        return pl.pallas_call(
            functools.partial(carry_kernel, part),
            out_shape=jax.ShapeDtypeStruct((2 * QUARTER, WIDTH), BF16),
            in_specs=[SMEM] + [VMEM] * 4 + [anywhere],
            out_specs=VMEM,
            compiler_params=room(12),
            cost_estimate=cost(2 * strip_flops, 4_000_000),
            name="carry",
        )(term_shift, site_own, site_pair, site_next, left, after)

    upper = carry(0, held)
    (far,) = pl.pallas_call(
        functools.partial(split_kernel, 0),
        out_shape=(piece,),
        in_specs=[VMEM, VMEM],
        out_specs=(VMEM,),
        compiler_params=room(6),
        cost_estimate=cost(PIECE * WIDTH, 8 * PIECE * WIDTH),
        name="split_first",
    )(held, moved_first)
    far_got = swap(far, far_route)
    ring, half, keep = pl.pallas_call(
        functools.partial(split_kernel, 1),
        out_shape=(piece, piece, jax.ShapeDtypeStruct((PIECE, WIDTH), F32)),
        in_specs=[VMEM, VMEM],
        out_specs=(VMEM, VMEM, VMEM),
        compiler_params=room(6),
        cost_estimate=cost(3 * PIECE * WIDTH, 24 * PIECE * WIDTH),
        name="split_second",
    )(held, moved_second)
    ring_got = swap(ring, stage_route(2))
    half_got = swap(half, stage_route(3))
    lower = carry(1, keep)
    renewed, done = pl.pallas_call(
        renew_kernel,
        out_shape=(square, jax.ShapeDtypeStruct((8, 128), F32)),
        in_specs=[SMEM, SMEM] + [VMEM] * 3 + [anywhere],
        out_specs=(HBM, VMEM),
        scratch_shapes=[pltpu.VMEM((WIDTH, WIDTH), BF16), pltpu.SemaphoreType.DMA((4,))],
        compiler_params=room(12),
        cost_estimate=cost(2 * WIDTH * WIDTH * WIDTH, 4_000_000),
        name="renew",
    )(sector_sizes, term_shift, upper, lower, turned, keep)
    applied = pl.pallas_call(
        finish_kernel,
        out_shape=jax.ShapeDtypeStruct((PIECE, WIDTH), F32),
        in_specs=[VMEM] * 4 + [pl.BlockSpec(memory_space=pl.ANY)],
        out_specs=VMEM,
        compiler_params=room(4),
        cost_estimate=cost(4 * PIECE * WIDTH, 8 * PIECE * WIDTH),
        name="finish",
    )(keep, far_got, ring_got, half_got, done)
    return applied[None], renewed[None, None]


def solution(mesh):
    placed = (
        P("sec", None, None),
        P("term", "sec", None, None),
        P("term", "sec", None, None),
        P("sec", None, None),
        P(),
        P("term"),
    )
    return jax.shard_map(
        shards,
        mesh=mesh,
        in_specs=placed,
        out_specs=(P("sec", "term", None), P("term", "sec", None, None)),
        check_vma=False,
    )
```

```python
import functools

import jax
import jax.numpy as jnp
from jax import lax
from jax.experimental import pallas as pl
from jax.experimental.pallas import tpu as pltpu
from jax.sharding import PartitionSpec as P


WIDTH = 768
TERMS = 16
SECTORS = 16
PIECE = WIDTH // TERMS
QUARTER = WIDTH // 4
SLOTS = (0, 4, 1, 2, 3, 5, 6, 7, 8, 9, 10, 11, 12, 13, 14, 15)
RELAYED = 160
DIRECT = WIDTH - 2 * RELAYED
RINGS = TERMS // 2
JUMPS = (1, -1, 3)
BF16 = jnp.bfloat16
F32 = jnp.float32
VMEM = pl.BlockSpec(memory_space=pltpu.VMEM)
SMEM = pl.BlockSpec(memory_space=pltpu.SMEM)
HBM = pl.BlockSpec(memory_space=pltpu.HBM)


def partner(stage, term, sector):
    ring, half = term // 2, term % 2
    if stage == 3:
        return 2 * ring + 1 - half
    sign = 1 - 2 * ((ring + sector) % 2)
    return 2 * ((ring + sign * JUMPS[stage] + RINGS) % RINGS) + half


def swap(block, where):
    route = []
    for term in range(TERMS):
        for sector in range(SECTORS):
            other_term, other_sector = where(term, sector)
            route.append((term * SECTORS + sector, other_term * SECTORS + other_sector))
    return lax.ppermute(block, ("term", "sec"), route)


def pair_sector(term, sector):
    return term, sector ^ 1


def next_sector(term, sector):
    return term, (sector + 1 if sector % 2 else sector - 1) % SECTORS


def stage_route(stage):
    return lambda term, sector: (partner(stage, term, sector), sector)


def far_route(term, sector):
    return partner(3, partner(2, term, sector), sector), sector


def sizes_here(sizes_ref, shift_ref):
    sector = lax.axis_index("sec")
    source = sector + shift_ref[0]
    inside = (source >= 0) & (source < SECTORS)
    source_size = jnp.where(inside, sizes_ref[jnp.clip(source, 0, SECTORS - 1)], 0)
    return sizes_ref[sector], source_size


def ones_below(size, start, count, dim):
    shape = (count, 1) if dim == 0 else (1, count)
    index = lax.broadcasted_iota(jnp.int32, shape, dim) + start
    return jnp.where(index < size, 1.0, 0.0).astype(BF16)


def piece_at(slot):
    term, sector = lax.axis_index("term"), lax.axis_index("sec")
    for stage in range(4):
        if not (slot >> (3 - stage)) & 1:
            term = partner(stage, term, sector)
    return term


def relay_starts():
    odd = (lax.axis_index("term") // 2 + lax.axis_index("sec")) % 2
    taken = DIRECT + RELAYED * odd
    passed = DIRECT + RELAYED * (1 - odd)
    return pl.multiple_of(taken, 16), pl.multiple_of(passed, 16)


def cut_kernel(state_ref, shared_out, direct_out, sems):
    others = relay_starts()[1]
    shared = pltpu.make_async_copy(state_ref.at[pl.ds(others, RELAYED), :], shared_out, sems.at[0])
    direct = pltpu.make_async_copy(state_ref.at[pl.ds(0, DIRECT), :], direct_out, sems.at[1])
    shared.start()
    direct.start()
    shared.wait()
    direct.wait()


def bring_kernel(state_ref, site_ref, out_ref, turned_out, sem):
    copy = pltpu.make_async_copy(state_ref, out_ref, sem)
    copy.start()
    turned_out[...] = site_ref[...].T
    copy.wait()


def prepare_kernel(
    sizes_ref,
    shift_ref,
    left_hbm,
    right_hbm,
    site_hbm,
    left_out,
    right_out,
    site_out,
    left_ref,
    right_ref,
    site_ref,
    sems,
):
    moves = ((left_hbm, left_ref), (right_hbm, right_ref), (site_hbm, site_ref))
    copies = [
        pltpu.make_async_copy(source, target, sems.at[index])
        for index, (source, target) in enumerate(moves)
    ]
    for copy in copies:
        copy.start()
    own, source = sizes_here(sizes_ref, shift_ref)
    own_columns = ones_below(own, 0, WIDTH, 1)
    source_columns = ones_below(source, 0, WIDTH, 1)
    for copy in copies:
        copy.wait()
    for place, slot in enumerate(SLOTS):
        start = pl.multiple_of(piece_at(slot) * PIECE, 16)
        here = pl.ds(place * PIECE, PIECE)
        rows = ones_below(own, start, PIECE, 0)
        left_out[here, :] = left_ref[pl.ds(start, PIECE), :] * rows * source_columns
        site_out[here, :] = site_ref[pl.ds(start, PIECE), :] * own_columns
        source_rows = ones_below(source, place * PIECE, PIECE, 0)
        right_out[here, :] = right_ref[here, :] * source_rows * own_columns


def with_source(shift_ref, own, pair, far):
    shift = shift_ref[0]
    even = lax.axis_index("sec") % 2 == 0
    local = shift == 0
    from_pair = (shift == 1) == even

    pl.when(local)(own)
    pl.when(jnp.logical_not(local) & from_pair)(pair)
    pl.when(jnp.logical_not(local) & jnp.logical_not(from_pair))(far)


def mix_kernel(
    shift_ref,
    own_ref,
    pair_ref,
    direct_ref,
    taken_ref,
    passed_ref,
    right_ref,
    left_ref,
    mixed_out,
    lead_out,
    send_out,
    joined_ref,
):
    def body(source_ref):
        mixed = jnp.dot(source_ref[...], right_ref[...], preferred_element_type=F32).astype(BF16)
        mixed_out[...] = mixed
        send = jnp.dot(left_ref[: 5 * PIECE, :], mixed, preferred_element_type=F32).astype(BF16)
        lead_out[...] = send[: 2 * PIECE, :]
        send_out[...] = send[2 * PIECE :, :]

    def joined():
        taken, passed = relay_starts()
        joined_ref[:DIRECT, :] = direct_ref[...]
        joined_ref[pl.ds(taken, RELAYED), :] = taken_ref[...]
        joined_ref[pl.ds(passed, RELAYED), :] = passed_ref[...]
        body(joined_ref)

    with_source(shift_ref, lambda: body(own_ref), lambda: body(pair_ref), joined)


def send_kernel(left_ref, mixed_ref, send_out):
    rows = left_ref[5 * PIECE : 8 * PIECE, :]
    send_out[...] = jnp.dot(rows, mixed_ref[...], preferred_element_type=F32).astype(BF16)


def keep_kernel(left_ref, mixed_ref, after_ref, first_out, second_out):
    del after_ref
    for part, out in ((2, first_out), (3, second_out)):
        rows = left_ref[part * QUARTER : (part + 1) * QUARTER, :]
        out[...] = jnp.dot(rows, mixed_ref[...], preferred_element_type=F32)


def pass_kernel(start, keep_ref, got_ref, out_ref):
    here = pl.ds(start, out_ref.shape[0])
    out_ref[...] = (keep_ref[here, :] + got_ref[: out_ref.shape[0], :].astype(F32)).astype(BF16)


def hold_kernel(keep_ref, got_ref, out_ref):
    out_ref[...] = keep_ref[PIECE:, :] + got_ref[...].astype(F32)


def far_kernel(keep_ref, lead_ref, moved_ref, out_ref):
    total = keep_ref[:PIECE, :] + lead_ref[PIECE:, :].astype(F32) + moved_ref[...].astype(F32)
    out_ref[...] = total.astype(BF16)


def split_kernel(hold_ref, got_ref, *outs):
    for slot, out in enumerate(outs):
        here = pl.ds(slot * PIECE, PIECE)
        out[...] = (hold_ref[here, :] + got_ref[here, :].astype(F32)).astype(out.dtype)


def finish_kernel(keep_ref, far_ref, ring_ref, half_ref, done_ref, out_ref):
    del done_ref
    total = keep_ref[...] + half_ref[...].astype(F32)
    out_ref[...] = total + (ring_ref[...].astype(F32) + far_ref[...].astype(F32))


def carry_kernel(part, shift_ref, own_ref, pair_ref, next_ref, left_ref, after_ref, out_ref):
    del after_ref
    rows = pl.ds(part * 2 * QUARTER, 2 * QUARTER)

    def body(source_ref):
        carried = jnp.dot(left_ref[rows, :], source_ref[...], preferred_element_type=F32)
        out_ref[...] = carried.astype(BF16)

    with_source(shift_ref, *(functools.partial(body, ref) for ref in (own_ref, pair_ref, next_ref)))


def renew_kernel(
    sizes_ref, shift_ref, upper_ref, lower_ref, site_ref, after_ref, out_hbm, done_ref, rows_ref, sems
):
    del after_ref
    done_ref[...] = jnp.zeros(done_ref.shape, F32)
    _, source_size = sizes_here(sizes_ref, shift_ref)
    columns = ones_below(source_size, 0, WIDTH, 1)
    carried = jnp.concatenate([upper_ref[...] * columns, lower_ref[...] * columns], axis=0)
    copies = []
    for part in range(4):
        here = pl.ds(part * QUARTER, QUARTER)
        renewed = jnp.dot(site_ref[here, :], carried, preferred_element_type=F32)
        rows_ref[here, :] = renewed.astype(BF16)
        copies.append(
            pltpu.make_async_copy(rows_ref.at[here, :], out_hbm.at[here, :], sems.at[part])
        )
        copies[-1].start()
    for copy in copies:
        copy.wait()


def room(mebibytes):
    return pltpu.CompilerParams(vmem_limit_bytes=mebibytes * 1024 * 1024)


def cost(flops, moved):
    return pl.CostEstimate(flops=flops, bytes_accessed=moved, transcendentals=0)


def shards(state, left_environment, right_environment, site_blocks, sector_sizes, term_shift):
    square = jax.ShapeDtypeStruct((WIDTH, WIDTH), BF16)
    state_own, site_own = state[0], site_blocks[0]
    shared, direct = pl.pallas_call(
        cut_kernel,
        out_shape=(
            jax.ShapeDtypeStruct((RELAYED, WIDTH), BF16),
            jax.ShapeDtypeStruct((DIRECT, WIDTH), BF16),
        ),
        in_specs=[HBM],
        out_specs=(VMEM, VMEM),
        scratch_shapes=[pltpu.SemaphoreType.DMA((2,))],
        compiler_params=room(4),
        cost_estimate=cost(1000, 2_000_000),
        name="cut",
    )(state_own)
    taken = swap(shared, next_sector)
    direct_got = swap(direct, next_sector)
    state_pair = swap(state_own, pair_sector)
    passed = swap(taken, stage_route(0))
    site_next = swap(site_own, next_sector)
    site_pair = swap(site_own, pair_sector)
    left, right, site = pl.pallas_call(
        prepare_kernel,
        out_shape=(square,) * 3,
        in_specs=[SMEM, SMEM] + [HBM] * 3,
        out_specs=(VMEM,) * 3,
        scratch_shapes=[pltpu.VMEM((WIDTH, WIDTH), BF16)] * 3 + [pltpu.SemaphoreType.DMA((3,))],
        compiler_params=room(12),
        cost_estimate=cost(6_000_000, 1000),
        name="prepare",
    )(sector_sizes, term_shift, left_environment[0, 0], right_environment[0, 0], site_own)
    state_here, turned = pl.pallas_call(
        bring_kernel,
        out_shape=(square, square),
        in_specs=[HBM, VMEM],
        out_specs=(VMEM, VMEM),
        scratch_shapes=[pltpu.SemaphoreType.DMA],
        compiler_params=room(10),
        cost_estimate=cost(1000, 2_400_000),
        name="bring",
    )(state_own, site)
    anywhere = pl.BlockSpec(memory_space=pl.ANY)
    strip_sum = jax.ShapeDtypeStruct((QUARTER, WIDTH), F32)
    piece = jax.ShapeDtypeStruct((PIECE, WIDTH), BF16)
    pieces = jax.ShapeDtypeStruct((3 * PIECE, WIDTH), BF16)
    strip_flops = 2 * QUARTER * WIDTH * WIDTH
    mixed, send_lead, send_first = pl.pallas_call(
        mix_kernel,
        out_shape=(square, jax.ShapeDtypeStruct((2 * PIECE, WIDTH), BF16), pieces),
        in_specs=[SMEM] + [VMEM] * 7,
        out_specs=(VMEM, VMEM, VMEM),
        scratch_shapes=[pltpu.VMEM((WIDTH, WIDTH), BF16)],
        compiler_params=room(20),
        cost_estimate=cost(5 * strip_flops, 6_000_000),
        name="mix",
    )(term_shift, state_here, state_pair, direct_got, taken, passed, right, left)
    got_lead = swap(send_lead, stage_route(0))
    got_first = swap(send_first, stage_route(0))
    send_second = pl.pallas_call(
        send_kernel,
        out_shape=pieces,
        in_specs=[VMEM, VMEM],
        out_specs=VMEM,
        compiler_params=room(12),
        cost_estimate=cost(strip_flops, 2_000_000),
        name="send",
    )(left, mixed)
    got_second = swap(send_second, stage_route(0))
    keep_first, keep_second = pl.pallas_call(
        keep_kernel,
        out_shape=(strip_sum, strip_sum),
        in_specs=[VMEM, VMEM, anywhere],
        out_specs=(VMEM, VMEM),
        compiler_params=room(12),
        cost_estimate=cost(2 * strip_flops, 3_000_000),
        name="keep",
    )(left, mixed, send_second)

    def passing(start, got, shape):
        return pl.pallas_call(
            functools.partial(pass_kernel, start),
            out_shape=shape,
            in_specs=[VMEM, VMEM],
            out_specs=VMEM,
            compiler_params=room(6),
            cost_estimate=cost(QUARTER * WIDTH, 8 * QUARTER * WIDTH),
            name="pass",
        )(keep_first, got)

    pass_first = passing(0, got_lead, piece)
    moved_first = swap(pass_first, stage_route(1))
    pass_second = passing(PIECE, got_first, pieces)
    moved_second = swap(pass_second, stage_route(1))
    held = pl.pallas_call(
        hold_kernel,
        out_shape=jax.ShapeDtypeStruct((3 * PIECE, WIDTH), F32),
        in_specs=[VMEM, VMEM],
        out_specs=VMEM,
        compiler_params=room(6),
        cost_estimate=cost(QUARTER * WIDTH, 8 * QUARTER * WIDTH),
        name="hold",
    )(keep_second, got_second)

    def carry(part, after):
        return pl.pallas_call(
            functools.partial(carry_kernel, part),
            out_shape=jax.ShapeDtypeStruct((2 * QUARTER, WIDTH), BF16),
            in_specs=[SMEM] + [VMEM] * 4 + [anywhere],
            out_specs=VMEM,
            compiler_params=room(12),
            cost_estimate=cost(2 * strip_flops, 4_000_000),
            name="carry",
        )(term_shift, site_own, site_pair, site_next, left, after)

    far = pl.pallas_call(
        far_kernel,
        out_shape=piece,
        in_specs=[VMEM] * 3,
        out_specs=VMEM,
        compiler_params=room(6),
        cost_estimate=cost(PIECE * WIDTH, 8 * PIECE * WIDTH),
        name="far",
    )(keep_second, got_lead, moved_first)
    far_got = swap(far, far_route)
    upper = carry(0, far)
    ring, half, keep = pl.pallas_call(
        split_kernel,
        out_shape=(piece, piece, jax.ShapeDtypeStruct((PIECE, WIDTH), F32)),
        in_specs=[VMEM, VMEM],
        out_specs=(VMEM, VMEM, VMEM),
        compiler_params=room(6),
        cost_estimate=cost(3 * PIECE * WIDTH, 24 * PIECE * WIDTH),
        name="split_second",
    )(held, moved_second)
    ring_got = swap(ring, stage_route(2))
    half_got = swap(half, stage_route(3))
    lower = carry(1, keep)
    renewed, done = pl.pallas_call(
        renew_kernel,
        out_shape=(square, jax.ShapeDtypeStruct((8, 128), F32)),
        in_specs=[SMEM, SMEM] + [VMEM] * 3 + [anywhere],
        out_specs=(HBM, VMEM),
        scratch_shapes=[pltpu.VMEM((WIDTH, WIDTH), BF16), pltpu.SemaphoreType.DMA((4,))],
        compiler_params=room(12),
        cost_estimate=cost(2 * WIDTH * WIDTH * WIDTH, 4_000_000),
        name="renew",
    )(sector_sizes, term_shift, upper, lower, turned, keep)
    applied = pl.pallas_call(
        finish_kernel,
        out_shape=jax.ShapeDtypeStruct((PIECE, WIDTH), F32),
        in_specs=[VMEM] * 4 + [pl.BlockSpec(memory_space=pl.ANY)],
        out_specs=VMEM,
        compiler_params=room(4),
        cost_estimate=cost(4 * PIECE * WIDTH, 8 * PIECE * WIDTH),
        name="finish",
    )(keep, far_got, ring_got, half_got, done)
    return applied[None], renewed[None, None]


def solution(mesh):
    placed = (
        P("sec", None, None),
        P("term", "sec", None, None),
        P("term", "sec", None, None),
        P("sec", None, None),
        P(),
        P("term"),
    )
    return jax.shard_map(
        shards,
        mesh=mesh,
        in_specs=placed,
        out_specs=(P("sec", "term", None), P("term", "sec", None, None)),
        check_vma=False,
    )
```
